32 devices in a mesh: layer: 8 (over y, x, core), tensor: 4 (over z).
Axes of the slice: x: 2, y: 2, z: 4, core: 2. Of those that a mesh axis runs over, the one named last changes fastest.
Arguments:
- gradient: bfloat16 [8, 1024, 8192], P(None, 'tensor', 'layer'), may hold values from -8 to 8
- row_basis: bfloat16 [8, 1024, 256], P('layer', 'tensor'), may hold values from -0.1875 to 0.1875
- column_basis: bfloat16 [8, 8192, 256], P('layer', 'tensor'), may hold values from -0.0625 to 0.0625
- row_eigen: float32 [8, 256], P('layer'), may hold values from 0.01 to 10
- column_eigen: float32 [8, 256], P('layer'), may hold values from 0.01 to 10
- row_escape: float32 [8], P('layer'), may hold values from 0.02 to 0.2
- column_escape: float32 [8], P('layer'), may hold values from 0.02 to 0.2
Outputs:
- update: bfloat16 [8, 1024, 8192], P(None, 'tensor', 'layer')
The draws below stay inside these ranges and needn't reach their ends.
All inputs are finite; a program needn't handle non-finite values.
Results may differ from the reference program's by a relative error of at most 0.0055.
Values may be sent and summed in bfloat16 or wider, within the bound.
A program may use at most 128 MiB of HBM per device.

```python
import math
import jax
import jax.numpy as jnp
from jax import lax

D = 8192
BLK = 1024
K = 256
LAYERS = 8


def draw_gradient(key, part):
    first, second, third, fourth = jax.random.split(jax.random.fold_in(key, 17), 4)
    noise = jax.random.normal(first, (LAYERS, BLK, D), jnp.float32)
    segment = jnp.exp(jax.random.uniform(third, (LAYERS, 1, D // 64), jnp.float32, math.log(0.4), math.log(2.5)))
    segment = jnp.repeat(segment, 64, axis=2)
    rowscale = jnp.exp(jax.random.uniform(second, (LAYERS, BLK, 1), jnp.float32, math.log(0.5), math.log(2.0)))
    values = rowscale * segment * noise
    return jnp.clip(values, -8.0, 8.0).astype(jnp.bfloat16)


def steps_of(stream_key, extent, shards, smallest, largest):
    factor_of = 1.0
    for dim, blocks in shards:
        heights = jax.random.uniform(jax.random.fold_in(jax.random.fold_in(stream_key, 6), dim), (blocks,), jnp.float32, smallest / len(shards), largest / len(shards))
        factor_of = factor_of * jnp.repeat(jnp.exp(heights), extent[dim] // blocks).reshape((-1,) + (1,) * (len(extent) - 1 - dim))
    return factor_of


def scatter_about(rng, dims, scale, bound, shards=(), dtype=jnp.bfloat16):
    values = jax.random.normal(rng, dims, jnp.float32) * scale
    if len(shards) > 0:
        values = steps_of(rng, dims, shards, -0.22, 0.18) * values
    return jnp.clip(values, min=-bound, max=bound).astype(dtype)


def setup_inputs(seed: int = 0) -> dict:
    keys = jax.random.split(jax.random.key(seed), 8)
    return {
        "gradient": draw_gradient(jax.random.fold_in(keys[7], 71), 0),
        "row_basis": scatter_about(keys[1], (LAYERS, BLK, K), BLK ** -0.5, 0.1875, ((0, 8), (1, 4))),
        "column_basis": scatter_about(keys[2], (LAYERS, D, K), D ** -0.5, 0.0625, ((0, 8), (1, 4))),
        "row_eigen": jnp.clip(jnp.exp(math.log(10.0) - 6.9077553 * jax.random.uniform(keys[3], (LAYERS, K), jnp.float32) ** steps_of(keys[3], (LAYERS, K), ((0, 8),), -0.2, 0.2)), 0.01, 10.0),
        "column_eigen": jnp.clip(jnp.exp(math.log(10.0) - 6.9077553 * jax.random.uniform(keys[4], (LAYERS, K), jnp.float32) ** steps_of(keys[4], (LAYERS, K), ((0, 8),), -0.2, 0.2)), 0.01, 10.0),
        "row_escape": jnp.clip(jnp.exp(math.log(0.2) - 2.3025851 * jax.random.uniform(keys[5], (LAYERS,), jnp.float32) ** steps_of(keys[5], (LAYERS,), ((0, 8),), -0.2, 0.2)), 0.02, 0.2),
        "column_escape": jnp.clip(jnp.exp(math.log(0.2) - 2.3025851 * jax.random.uniform(keys[6], (LAYERS,), jnp.float32) ** steps_of(keys[6], (LAYERS,), ((0, 8),), -0.2, 0.2)), 0.02, 0.2),
    }


def one_layer(operands):
    block_grad, basis_rows, basis_columns, eigen_rows, eigen_columns, escape_rows, escape_columns = operands
    row_base = escape_rows ** (-0.25)
    column_base = escape_columns ** (-0.25)
    row_coef = (eigen_rows + escape_rows) ** (-0.25) - row_base
    column_coef = (eigen_columns + escape_columns) ** (-0.25) - column_base
    projected = jnp.dot(basis_rows.T, block_grad, preferred_element_type=jnp.float32)
    scaled = (row_coef[:, None] * projected).astype(jnp.bfloat16)
    core = jnp.dot(scaled, basis_columns, preferred_element_type=jnp.float32).astype(jnp.bfloat16)
    middle = jnp.dot(block_grad, basis_columns, preferred_element_type=jnp.float32)
    left_factor = ((row_base * middle + jnp.dot(basis_rows, core, preferred_element_type=jnp.float32)) * column_coef[None, :]).astype(jnp.bfloat16)
    raw_update = row_base * column_base * block_grad.astype(jnp.float32)
    raw_update = raw_update + column_base * jnp.dot(basis_rows, scaled, preferred_element_type=jnp.float32)
    raw_update = raw_update + jnp.dot(left_factor, basis_columns.T, preferred_element_type=jnp.float32)
    grad_sq = jnp.sum(jnp.square(block_grad.astype(jnp.float32)))
    update_sq = jnp.sum(jnp.square(raw_update))
    return (raw_update * jnp.sqrt((grad_sq + 1.0) / (update_sq + 1.0))).astype(jnp.bfloat16)

def reference(gradient, row_basis, column_basis, row_eigen, column_eigen, row_escape, column_escape):
    return lax.map(one_layer, (gradient, row_basis, column_basis, row_eigen, column_eigen, row_escape, column_escape))
```

```python
import functools

import jax
import jax.numpy as jnp
from jax import lax
from jax.experimental import pallas as pl
from jax.experimental.pallas import tpu as pltpu
from jax.sharding import PartitionSpec as P

MESH = pl.DeviceIdType.MESH
F32 = jnp.float32
BF16 = jnp.bfloat16


def remote(src, dst, send, recv, axis, index):
    return pltpu.make_async_remote_copy(
        src_ref=src,
        dst_ref=dst,
        send_sem=send,
        recv_sem=recv,
        device_id={axis: index},
        device_id_type=MESH,
    )


def loop(lo, hi, fn):
    def step(i, carry):
        fn(i)
        return carry

    lax.fori_loop(lo, hi, step, 0)


def dot(a, b):
    return jnp.dot(a, b, preferred_element_type=F32)


def kernel(
    L, T,
    g, rows_basis, rows_basis_t, cols, dr, dc, base,
    out,
    gg, own, pin, qin, pout, qout, call, mid, left, core_out, core_in, raw_out, raw_in,
    gacc, uacc, nsend, nrecv, fsend, frecv,
    gs, gr, cs, cr, ps, pr, qs, qr, ks, kr, os_, or_, ns, nr, fs, fr,
):
    me = lax.axis_index("layer")
    t = lax.axis_index("tensor")
    W = g.shape[2]
    Cr = cols.shape[0]
    right, lft = t + 1, t - 1
    has_right, has_left = t < T - 1, t > 0

    barrier = pltpu.get_barrier_semaphore()
    loop(1, L, lambda d: pl.semaphore_signal(
        barrier, inc=1, device_id={"layer": lax.rem(me + d, L)}, device_id_type=MESH))
    loop(1, T, lambda d: pl.semaphore_signal(
        barrier, inc=1, device_id={"tensor": lax.rem(t + d, T)}, device_id_type=MESH))
    pl.semaphore_wait(barrier, L + T - 2)

    def g_copy(slot, dst):
        return remote(g.at[dst], gg.at[slot], gs.at[dst], gr.at[slot], "layer", dst)

    def c_rows(s):
        return call.at[pl.ds(pl.multiple_of(s * Cr, Cr), Cr)]

    def c_copy(src, s, h, side):
        return remote(src, c_rows(s), cs.at[side, h], cr.at[s], "tensor", right if side == 0 else lft)

    pl.when(has_right)(lambda: c_copy(cols, t, 0, 0).start())
    pl.when(has_left)(lambda: c_copy(cols, t, 0, 1).start())
    loop(1, L, lambda d: g_copy(me, lax.rem(me + d, L)).start())
    gg[me] = g[me]
    call[pl.ds(pl.multiple_of(t * Cr, Cr), Cr), :] = cols[...]
    gacc[...] = jnp.zeros_like(gacc)
    uacc[...] = jnp.zeros_like(uacc)
    mid[...] = jnp.zeros_like(mid)

    @pl.when(t == 0)
    def _():
        loop(0, L, lambda d: pin.__setitem__(d, jnp.zeros(pin.shape[1:], BF16)))

    @pl.when(t == T - 1)
    def _():
        loop(0, L, lambda d: qin.__setitem__(d, jnp.zeros(qin.shape[1:], BF16)))

    def c_hop(h):
        @pl.when(t - h >= 0)
        def _():
            c_copy(cols, t - h, 0, 0).wait_recv()
            pl.when(has_right)(lambda: c_copy(c_rows(t - h), t - h, h, 0).start())

        @pl.when(t + h < T)
        def _():
            c_copy(cols, t + h, 0, 1).wait_recv()
            pl.when(has_left)(lambda: c_copy(c_rows(t + h), t + h, h, 1).start())

    def p_copy(src, d):
        return remote(src, pin.at[d], ps.at[d], pr.at[d], "tensor", right)

    def q_copy(src, d):
        return remote(src, qin.at[d], qs.at[d], qr.at[d], "tensor", lft)

    def s_step(k):
        d = k - t

        @pl.when((d >= 0) & (d < L))
        def _():
            @pl.when(t == 0)
            def _():
                p_copy(own.at[d], d).start()

            @pl.when(has_left)
            def _():
                p_copy(own.at[d], d).wait_recv()

                @pl.when(has_right)
                def _():
                    pout[d] = (pin[d].astype(F32) + own[d].astype(F32)).astype(BF16)
                    p_copy(pout.at[d], d).start()

        e = k - (T - 1 - t)

        @pl.when((e >= 0) & (e < L))
        def _():
            @pl.when(t == T - 1)
            def _():
                q_copy(own.at[e], e).start()

            @pl.when(has_right)
            def _():
                q_copy(own.at[e], e).wait_recv()

                @pl.when(has_left)
                def _():
                    qout[e] = (qin[e].astype(F32) + own[e].astype(F32)).astype(BF16)
                    q_copy(qout.at[e], e).start()

    half = L // 2

    def arrive(d):
        j = lax.rem(me - d + L, L)
        pl.when(d > 0)(lambda: g_copy(j, j).wait_recv())
        block = gg[j]
        own[d] = dot(rows_basis_t[...], block).astype(BF16)
        wide = block.astype(F32)
        gacc[...] += jnp.sum(wide * wide, axis=0, keepdims=True)
        for h in range(1, T - 1):
            pl.when(d == (h * L) // (T - 1))(lambda h=h: c_hop(h))
        pl.when(d < half)(lambda: s_step(d))

    loop(0, L, arrive)
    c_hop(T - 1)

    def mid_step(j):
        mid[...] += dot(gg[j], call[pl.ds(pl.multiple_of(j * W, W), W), :])

    loop(0, L, mid_step)
    core_out[...] = dot(rows_basis_t[...], mid[...].astype(BF16)).astype(BF16)

    def k_copy(slot, dst):
        return remote(core_out, core_in.at[slot], ks.at[dst], kr.at[slot], "tensor", dst)

    loop(1, T, lambda d: k_copy(t, lax.rem(t + d, T)).start())
    core_in[t] = core_out[...]
    s_step(half)
    for d in range(1, T):
        s = lax.rem(t + d, T)
        k_copy(s, s).wait_recv()
    core = core_in[0].astype(F32)
    for s in range(1, T):
        core = core + core_in[s].astype(F32)
    core = (core * dr[:, :1]).astype(BF16)
    mixed = base[0:1, 0:1] * mid[...] + dot(rows_basis[...], core)
    left[...] = (mixed * dc[0:1, :]).astype(BF16)

    def o_copy(slot, dst):
        return remote(raw_out.at[dst], raw_in.at[slot], os_.at[dst], or_.at[slot], "layer", dst)

    def emit(d):
        j = lax.rem(me - d + L, L)
        total = own[d].astype(F32) + pin[d].astype(F32) + qin[d].astype(F32)
        scaled = (total * dr[:, :1]).astype(BF16)
        raw = base[2:3, 0:1] * gg[j].astype(F32)
        raw = raw + base[1:2, 0:1] * dot(rows_basis[...], scaled)
        raw = raw + lax.dot_general(
            left[...], call[pl.ds(pl.multiple_of(j * W, W), W), :],
            (((1,), (1,)), ((), ())), preferred_element_type=F32)
        uacc[...] += jnp.sum(raw * raw, axis=0, keepdims=True)

        @pl.when(d == 0)
        def _():
            raw_in[me] = raw.astype(BF16)

        @pl.when(d > 0)
        def _():
            raw_out[j] = raw.astype(BF16)
            o_copy(me, j).start()

    last = T - 1

    def tail_step(k):
        pl.when(k > half)(lambda: s_step(k))
        pl.when(k - last >= 0)(lambda: emit(k - last))

    loop(min(last, half + 1), L + last, tail_step)

    nsend[0:8, :] = jnp.broadcast_to(jnp.sum(gacc[...]), (8, 128))
    nsend[8:16, :] = jnp.broadcast_to(jnp.sum(uacc[...]), (8, 128))

    def n_copy(slot, dst):
        return remote(nsend, nrecv.at[slot], ns.at[dst], nr.at[slot], "tensor", dst)

    loop(1, T, lambda d: n_copy(t, lax.rem(t + d, T)).start())
    nrecv[t] = nsend[...]
    for d in range(1, T):
        s = lax.rem(t + d, T)
        n_copy(s, s).wait_recv()
    sq = nrecv[0]
    for s in range(1, T):
        sq = sq + nrecv[s]
    fsend[...] = jnp.sqrt((sq[0:8] + 1.0) / (sq[8:16] + 1.0))

    def f_copy(slot, dst):
        return remote(fsend, frecv.at[slot], fs.at[dst], fr.at[slot], "layer", dst)

    loop(1, L, lambda d: f_copy(me, lax.rem(me + d, L)).start())
    frecv[me] = fsend[...]

    def finish(d):
        j = lax.rem(me + d, L)

        @pl.when(d > 0)
        def _():
            o_copy(j, j).wait_recv()
            f_copy(j, j).wait_recv()

        out[j] = (raw_in[j].astype(F32) * frecv[j][0:1, 0:1]).astype(BF16)

    loop(0, L, finish)

    def drain_layer(d):
        j = lax.rem(me + d, L)
        g_copy(me, j).wait_send()
        o_copy(me, j).wait_send()
        f_copy(me, j).wait_send()

    loop(1, L, drain_layer)

    def drain_tensor(d):
        s = lax.rem(t + d, T)
        k_copy(t, s).wait_send()
        n_copy(t, s).wait_send()

    loop(1, T, drain_tensor)

    def drain_line(d):
        pl.when(has_right)(lambda: p_copy(own.at[d], d).wait_send())
        pl.when(has_left)(lambda: q_copy(own.at[d], d).wait_send())

    loop(0, L, drain_line)
    for h in range(T - 1):
        pl.when((t - h >= 0) & has_right)(lambda h=h: c_copy(cols, t, h, 0).wait_send())
        pl.when((t + h < T) & has_left)(lambda h=h: c_copy(cols, t, h, 1).wait_send())


def solution(mesh):
    L, T = mesh.shape["layer"], mesh.shape["tensor"]

    def body(gradient, row_basis, column_basis, row_eigen, column_eigen, row_escape, column_escape):
        row_base = row_escape ** (-0.25)
        column_base = column_escape ** (-0.25)
        row_coef = (row_eigen + row_escape[:, None]) ** (-0.25) - row_base[:, None]
        column_coef = (column_eigen + column_escape[:, None]) ** (-0.25) - column_base[:, None]
        _, r, W = gradient.shape
        _, Cr, K = column_basis.shape
        dr = jnp.broadcast_to(row_coef[0][:, None], (K, 128))
        dc = jnp.broadcast_to(column_coef, (8, K))
        base = jnp.broadcast_to(
            jnp.concatenate([row_base, column_base, row_base * column_base] + [row_base] * 5)[:, None], (8, 128))
        vmem = pl.BlockSpec(memory_space=pltpu.VMEM)
        chunk = pltpu.VMEM((L, K, W), BF16)
        block = pltpu.VMEM((L, r, W), BF16)
        sem = pltpu.SemaphoreType.DMA
        return pl.pallas_call(
            functools.partial(kernel, L, T),
            out_shape=jax.ShapeDtypeStruct((L, r, W), BF16),
            in_specs=[vmem] * 7,
            out_specs=vmem,
            scratch_shapes=[
                block, chunk, chunk, chunk, chunk, chunk,
                pltpu.VMEM((T * Cr, K), BF16),
                pltpu.VMEM((r, K), F32),
                pltpu.VMEM((r, K), BF16),
                pltpu.VMEM((K, K), BF16),
                pltpu.VMEM((T, K, K), BF16),
                block, block,
                pltpu.VMEM((1, W), F32),
                pltpu.VMEM((1, W), F32),
                pltpu.VMEM((16, 128), F32),
                pltpu.VMEM((T, 16, 128), F32),
                pltpu.VMEM((8, 128), F32),
                pltpu.VMEM((L, 8, 128), F32),
                sem((L,)), sem((L,)),
                sem((2, T)), sem((T,)),
                sem((L,)), sem((L,)),
                sem((L,)), sem((L,)),
                sem((T,)), sem((T,)),
                sem((L,)), sem((L,)),
                sem((T,)), sem((T,)),
                sem((L,)), sem((L,)),
            ],
            compiler_params=pltpu.CompilerParams(
                collective_id=0, has_side_effects=True, vmem_limit_bytes=62 * 1024 * 1024),
        )(gradient, row_basis[0], row_basis[0].T, column_basis[0], dr, dc, base)

    in_specs = (
        P(None, "tensor", "layer"),
        P("layer", "tensor", None),
        P("layer", "tensor", None),
        P("layer", None),
        P("layer", None),
        P("layer"),
        P("layer"),
    )
    out_specs = P(None, "tensor", "layer")
    return jax.shard_map(body, mesh=mesh, in_specs=in_specs, out_specs=out_specs, check_vma=False)
```

```python
import functools

import jax
import jax.numpy as jnp
from jax import lax
from jax.experimental import pallas as pl
from jax.experimental.pallas import tpu as pltpu
from jax.sharding import PartitionSpec as P

MESH = pl.DeviceIdType.MESH
F32 = jnp.float32
BF16 = jnp.bfloat16


def remote(src, dst, send, recv, axis, index):
    return pltpu.make_async_remote_copy(
        src_ref=src,
        dst_ref=dst,
        send_sem=send,
        recv_sem=recv,
        device_id={axis: index},
        device_id_type=MESH,
    )


def loop(lo, hi, fn):
    def step(i, carry):
        fn(i)
        return carry

    lax.fori_loop(lo, hi, step, 0)


def dot(a, b):
    return jnp.dot(a, b, preferred_element_type=F32)


def kernel(
    L, T,
    g, rows_basis, rows_basis_t, cols, dr, dc, base,
    out, factor,
    gg, own, pin, qin, pout, qout, call, mid, left, core_out, core_in, core_sum, raw_out,
    gacc, uacc, nsend, nrecv, fsend, frecv,
    gs, gr, cs, cr, ps, pr, qs, qr, ks, kr, os_, or_, ns, nr, fs, fr,
):
    me = lax.axis_index("layer")
    t = lax.axis_index("tensor")
    W = g.shape[2]
    Cr = cols.shape[0]
    right, lft = t + 1, t - 1
    has_right, has_left = t < T - 1, t > 0

    barrier = pltpu.get_barrier_semaphore()
    loop(1, L, lambda d: pl.semaphore_signal(
        barrier, inc=1, device_id={"layer": lax.rem(me + d, L)}, device_id_type=MESH))
    loop(1, T, lambda d: pl.semaphore_signal(
        barrier, inc=1, device_id={"tensor": lax.rem(t + d, T)}, device_id_type=MESH))
    pl.semaphore_wait(barrier, L + T - 2)

    def g_copy(slot, dst):
        return remote(g.at[dst], gg.at[slot], gs.at[dst], gr.at[slot], "layer", dst)

    def c_rows(s):
        return call.at[pl.ds(pl.multiple_of(s * Cr, Cr), Cr)]

    def c_copy(src, s, h, side):
        return remote(src, c_rows(s), cs.at[side, h], cr.at[s], "tensor", right if side == 0 else lft)

    pl.when(has_right)(lambda: c_copy(cols, t, 0, 0).start())
    pl.when(has_left)(lambda: c_copy(cols, t, 0, 1).start())
    loop(1, L, lambda d: g_copy(me, lax.rem(me + d, L)).start())
    gg[me] = g[me]
    call[pl.ds(pl.multiple_of(t * Cr, Cr), Cr), :] = cols[...]
    gacc[...] = jnp.zeros_like(gacc)
    uacc[...] = jnp.zeros_like(uacc)
    mid[...] = jnp.zeros_like(mid)

    @pl.when(t == 0)
    def _():
        loop(0, L, lambda d: pin.__setitem__(d, jnp.zeros(pin.shape[1:], BF16)))

    @pl.when(t == T - 1)
    def _():
        loop(0, L, lambda d: qin.__setitem__(d, jnp.zeros(qin.shape[1:], BF16)))

    def c_hop(h):
        @pl.when(t - h >= 0)
        def _():
            c_copy(cols, t - h, 0, 0).wait_recv()
            pl.when(has_right)(lambda: c_copy(c_rows(t - h), t - h, h, 0).start())

        @pl.when(t + h < T)
        def _():
            c_copy(cols, t + h, 0, 1).wait_recv()
            pl.when(has_left)(lambda: c_copy(c_rows(t + h), t + h, h, 1).start())

    def p_copy(src, d):
        return remote(src, pin.at[d], ps.at[d], pr.at[d], "tensor", right)

    def q_copy(src, d):
        return remote(src, qin.at[d], qs.at[d], qr.at[d], "tensor", lft)

    def end_send(d):
        pl.when(t == 0)(lambda: p_copy(own.at[d], d).start())
        pl.when(t == T - 1)(lambda: q_copy(own.at[d], d).start())

    def forward(k):
        d = k - t

        @pl.when((d >= 0) & (d < L) & has_left)
        def _():
            p_copy(own.at[d], d).wait_recv()

            @pl.when(has_right)
            def _():
                pout[d] = (pin[d].astype(F32) + own[d].astype(F32)).astype(BF16)
                p_copy(pout.at[d], d).start()

        e = k - (T - 1 - t)

        @pl.when((e >= 0) & (e < L) & has_right)
        def _():
            q_copy(own.at[e], e).wait_recv()

            @pl.when(has_left)
            def _():
                qout[e] = (qin[e].astype(F32) + own[e].astype(F32)).astype(BF16)
                q_copy(qout.at[e], e).start()

    half = L // 2
    early = ((T - 2) * L) // (T - 1) + 1

    def arrive(d):
        j = lax.rem(me - d + L, L)
        pl.when(d > 0)(lambda: g_copy(j, j).wait_recv())
        block = gg[j]
        own[d] = dot(rows_basis_t[...], block).astype(BF16)
        pl.when(d < half)(lambda: end_send(d))
        wide = block.astype(F32)
        gacc[...] += jnp.sum(wide * wide, axis=0, keepdims=True)
        for h in range(1, T - 1):
            pl.when(d == (h * L) // (T - 1))(lambda h=h: c_hop(h))
        pl.when(d >= early)(lambda: forward(d - early + 1))

    loop(0, L, arrive)
    c_hop(T - 1)

    def mid_step(j):
        mid[...] += dot(gg[j], call[pl.ds(pl.multiple_of(j * W, W), W), :])

    loop(0, L, mid_step)
    core_out[...] = dot(rows_basis_t[...], mid[...].astype(BF16)).astype(BF16)

    def kp_copy(src):
        return remote(src, core_in.at[0], ks.at[0], kr.at[0], "tensor", right)

    def kq_copy(src):
        return remote(src, core_in.at[1], ks.at[1], kr.at[1], "tensor", lft)

    @pl.when(t == 0)
    def _():
        core_in[0] = jnp.zeros(core_out.shape, BF16)
        kp_copy(core_out).start()

    @pl.when(t == T - 1)
    def _():
        core_in[1] = jnp.zeros(core_out.shape, BF16)
        kq_copy(core_out).start()

    loop(half, L, end_send)

    def core_step(k):
        @pl.when((k == half + t) & has_left)
        def _():
            kp_copy(core_out).wait_recv()

            @pl.when(has_right)
            def _():
                core_sum[0] = (core_in[0].astype(F32) + core_out[...].astype(F32)).astype(BF16)
                kp_copy(core_sum.at[0]).start()

        @pl.when((k == half + T - 1 - t) & has_right)
        def _():
            kq_copy(core_out).wait_recv()

            @pl.when(has_left)
            def _():
                core_sum[1] = (core_in[1].astype(F32) + core_out[...].astype(F32)).astype(BF16)
                kq_copy(core_sum.at[1]).start()

    def make_left():
        core = core_in[0].astype(F32) + core_in[1].astype(F32) + core_out[...].astype(F32)
        core = (core * dr[:, :1]).astype(BF16)
        mixed = base[0:1, 0:1] * mid[...] + dot(rows_basis[...], core)
        left[...] = (mixed * dc[0:1, :]).astype(BF16)

    def o_copy(slot, dst):
        return remote(raw_out.at[dst], out.at[slot], os_.at[dst], or_.at[slot], "layer", dst)

    def own_copy():
        return pltpu.make_async_copy(raw_out.at[me], out.at[me], os_.at[me])

    def emit(d):
        j = lax.rem(me - d + L, L)
        total = own[d].astype(F32) + pin[d].astype(F32) + qin[d].astype(F32)
        scaled = (total * dr[:, :1]).astype(BF16)
        raw = base[2:3, 0:1] * gg[j].astype(F32)
        raw = raw + base[1:2, 0:1] * dot(rows_basis[...], scaled)
        raw = raw + lax.dot_general(
            left[...], call[pl.ds(pl.multiple_of(j * W, W), W), :],
            (((1,), (1,)), ((), ())), preferred_element_type=F32)
        raw_out[j] = raw.astype(BF16)
        pl.when(d == 0)(lambda: own_copy().start())
        pl.when(d > 0)(lambda: o_copy(me, j).start())
        uacc[...] += jnp.sum(raw * raw, axis=0, keepdims=True)

    first = half + T - 1

    def upto(k):
        return jnp.minimum(k - T + 2, 3 + 2 * (k - first))

    def tail_step(k):
        core_step(k)
        forward(k)
        pl.when(k == first)(make_left)
        pl.when(k == first)(lambda: loop(0, upto(k), emit))
        pl.when(k > first)(lambda: loop(upto(k - 1), upto(k), emit))

    loop(L - early + 1, L + T - 1, tail_step)

    nsend[0:8, :] = jnp.broadcast_to(jnp.sum(gacc[...]), (8, 128))
    nsend[8:16, :] = jnp.broadcast_to(jnp.sum(uacc[...]), (8, 128))

    def n_copy(slot, dst):
        return remote(nsend, nrecv.at[slot], ns.at[dst], nr.at[slot], "tensor", dst)

    loop(1, T, lambda d: n_copy(t, lax.rem(t + d, T)).start())
    nrecv[t] = nsend[...]
    for d in range(1, T):
        s = lax.rem(t + d, T)
        n_copy(s, s).wait_recv()
    sq = nrecv[0]
    for s in range(1, T):
        sq = sq + nrecv[s]
    fsend[...] = jnp.sqrt((sq[0:8] + 1.0) / (sq[8:16] + 1.0))

    def f_copy(slot, dst):
        return remote(fsend, frecv.at[slot], fs.at[dst], fr.at[slot], "layer", dst)

    loop(1, L, lambda d: f_copy(me, lax.rem(me + d, L)).start())
    frecv[me] = fsend[...]
    own_copy().wait()

    def finish(d):
        j = lax.rem(me + d, L)
        o_copy(j, j).wait_recv()
        f_copy(j, j).wait_recv()

    loop(1, L, finish)
    factor[...] = frecv[...]

    def drain_layer(d):
        j = lax.rem(me + d, L)
        g_copy(me, j).wait_send()
        o_copy(me, j).wait_send()
        f_copy(me, j).wait_send()

    loop(1, L, drain_layer)
    pl.when(has_right)(lambda: kp_copy(core_out).wait_send())
    pl.when(has_left)(lambda: kq_copy(core_out).wait_send())

    def drain_tensor(d):
        s = lax.rem(t + d, T)
        n_copy(t, s).wait_send()

    loop(1, T, drain_tensor)

    def drain_line(d):
        pl.when(has_right)(lambda: p_copy(own.at[d], d).wait_send())
        pl.when(has_left)(lambda: q_copy(own.at[d], d).wait_send())

    loop(0, L, drain_line)
    for h in range(T - 1):
        pl.when((t - h >= 0) & has_right)(lambda h=h: c_copy(cols, t, h, 0).wait_send())
        pl.when((t + h < T) & has_left)(lambda h=h: c_copy(cols, t, h, 1).wait_send())


def solution(mesh):
    L, T = mesh.shape["layer"], mesh.shape["tensor"]

    def body(gradient, row_basis, column_basis, row_eigen, column_eigen, row_escape, column_escape):
        row_base = row_escape ** (-0.25)
        column_base = column_escape ** (-0.25)
        row_coef = (row_eigen + row_escape[:, None]) ** (-0.25) - row_base[:, None]
        column_coef = (column_eigen + column_escape[:, None]) ** (-0.25) - column_base[:, None]
        _, r, W = gradient.shape
        _, Cr, K = column_basis.shape
        dr = jnp.broadcast_to(row_coef[0][:, None], (K, 128))
        dc = jnp.broadcast_to(column_coef, (8, K))
        base = jnp.broadcast_to(
            jnp.concatenate([row_base, column_base, row_base * column_base] + [row_base] * 5)[:, None], (8, 128))
        vmem = pl.BlockSpec(memory_space=pltpu.VMEM)
        chunk = pltpu.VMEM((L, K, W), BF16)
        block = pltpu.VMEM((L, r, W), BF16)
        sem = pltpu.SemaphoreType.DMA
        raw, factor = pl.pallas_call(
            functools.partial(kernel, L, T),
            out_shape=(jax.ShapeDtypeStruct((L, r, W), BF16), jax.ShapeDtypeStruct((L, 8, 128), F32)),
            in_specs=[vmem] * 7,
            out_specs=(pl.BlockSpec(memory_space=pl.ANY), vmem),
            scratch_shapes=[
                block, chunk, chunk, chunk, chunk, chunk,
                pltpu.VMEM((T * Cr, K), BF16),
                pltpu.VMEM((r, K), F32),
                pltpu.VMEM((r, K), BF16),
                pltpu.VMEM((K, K), BF16),
                pltpu.VMEM((2, K, K), BF16),
                pltpu.VMEM((2, K, K), BF16),
                block,
                pltpu.VMEM((1, W), F32),
                pltpu.VMEM((1, W), F32),
                pltpu.VMEM((16, 128), F32),
                pltpu.VMEM((T, 16, 128), F32),
                pltpu.VMEM((8, 128), F32),
                pltpu.VMEM((L, 8, 128), F32),
                sem((L,)), sem((L,)),
                sem((2, T)), sem((T,)),
                sem((L,)), sem((L,)),
                sem((L,)), sem((L,)),
                sem((2,)), sem((2,)),
                sem((L,)), sem((L,)),
                sem((T,)), sem((T,)),
                sem((L,)), sem((L,)),
            ],
            compiler_params=pltpu.CompilerParams(
                collective_id=0, has_side_effects=True, vmem_limit_bytes=62 * 1024 * 1024),
        )(gradient, row_basis[0], row_basis[0].T, column_basis[0], dr, dc, base)
        return (raw.astype(F32) * factor[:, :1, :1]).astype(BF16)

    in_specs = (
        P(None, "tensor", "layer"),
        P("layer", "tensor", None),
        P("layer", "tensor", None),
        P("layer", None),
        P("layer", None),
        P("layer"),
        P("layer"),
    )
    out_specs = P(None, "tensor", "layer")
    return jax.shard_map(body, mesh=mesh, in_specs=in_specs, out_specs=out_specs, check_vma=False)
```

```python
import functools

import jax
import jax.numpy as jnp
from jax import lax
from jax.experimental import pallas as pl
from jax.experimental.pallas import tpu as pltpu
from jax.sharding import PartitionSpec as P

MESH = pl.DeviceIdType.MESH
F32 = jnp.float32
BF16 = jnp.bfloat16


def remote(src, dst, send, recv, axis, index):
    return pltpu.make_async_remote_copy(
        src_ref=src,
        dst_ref=dst,
        send_sem=send,
        recv_sem=recv,
        device_id={axis: index},
        device_id_type=MESH,
    )


def loop(lo, hi, fn):
    def step(i, carry):
        fn(i)
        return carry

    lax.fori_loop(lo, hi, step, 0)


def dot(a, b):
    return jnp.dot(a, b, preferred_element_type=F32)


def kernel(
    L, T,
    g, rows_basis, rows_basis_t, cols, dr, dc, base,
    out, factor,
    gg, own, pin, qin, pout, qout, call, mid, left, core_out, core_in, core_sum, raw_out,
    gacc, uacc, nsend, nrecv, fsend, frecv,
    gs, gr, cs, cr, ps, pr, qs, qr, ks, kr, os_, or_, ns, nr, fs, fr,
):
    me = lax.axis_index("layer")
    t = lax.axis_index("tensor")
    W = g.shape[2]
    Cr = cols.shape[0]
    right, lft = t + 1, t - 1
    has_right, has_left = t < T - 1, t > 0

    barrier = pltpu.get_barrier_semaphore()
    loop(1, L, lambda d: pl.semaphore_signal(
        barrier, inc=1, device_id={"layer": lax.rem(me + d, L)}, device_id_type=MESH))
    loop(1, T, lambda d: pl.semaphore_signal(
        barrier, inc=1, device_id={"tensor": lax.rem(t + d, T)}, device_id_type=MESH))
    pl.semaphore_wait(barrier, L + T - 2)

    def g_copy(slot, dst):
        return remote(g.at[dst], gg.at[slot], gs.at[dst], gr.at[slot], "layer", dst)

    def c_rows(s):
        return call.at[pl.ds(pl.multiple_of(s * Cr, Cr), Cr)]

    def c_copy(src, s, h, side):
        return remote(src, c_rows(s), cs.at[side, h], cr.at[s], "tensor", right if side == 0 else lft)

    pl.when(has_right)(lambda: c_copy(cols, t, 0, 0).start())
    pl.when(has_left)(lambda: c_copy(cols, t, 0, 1).start())
    loop(1, L, lambda d: g_copy(me, lax.rem(me + d, L)).start())
    gg[me] = g[me]
    call[pl.ds(pl.multiple_of(t * Cr, Cr), Cr), :] = cols[...]
    gacc[...] = jnp.zeros_like(gacc)
    uacc[...] = jnp.zeros_like(uacc)
    mid[...] = jnp.zeros_like(mid)

    @pl.when(t == 0)
    def _():
        loop(0, L, lambda d: pin.__setitem__(d, jnp.zeros(pin.shape[1:], BF16)))

    @pl.when(t == T - 1)
    def _():
        loop(0, L, lambda d: qin.__setitem__(d, jnp.zeros(qin.shape[1:], BF16)))

    def c_hop(h):
        @pl.when(t - h >= 0)
        def _():
            c_copy(cols, t - h, 0, 0).wait_recv()
            pl.when(has_right)(lambda: c_copy(c_rows(t - h), t - h, h, 0).start())

        @pl.when(t + h < T)
        def _():
            c_copy(cols, t + h, 0, 1).wait_recv()
            pl.when(has_left)(lambda: c_copy(c_rows(t + h), t + h, h, 1).start())

    def p_copy(src, d):
        return remote(src, pin.at[d], ps.at[d], pr.at[d], "tensor", right)

    def q_copy(src, d):
        return remote(src, qin.at[d], qs.at[d], qr.at[d], "tensor", lft)

    def end_send(d):
        pl.when(t == 0)(lambda: p_copy(own.at[d], d).start())
        pl.when(t == T - 1)(lambda: q_copy(own.at[d], d).start())

    def forward(k):
        d = k - t

        @pl.when((d >= 0) & (d < L) & has_left)
        def _():
            p_copy(own.at[d], d).wait_recv()

            @pl.when(has_right)
            def _():
                pout[d] = (pin[d].astype(F32) + own[d].astype(F32)).astype(BF16)
                p_copy(pout.at[d], d).start()

        e = k - (T - 1 - t)

        @pl.when((e >= 0) & (e < L) & has_right)
        def _():
            q_copy(own.at[e], e).wait_recv()

            @pl.when(has_left)
            def _():
                qout[e] = (qin[e].astype(F32) + own[e].astype(F32)).astype(BF16)
                q_copy(qout.at[e], e).start()

    half = L // 2
    early = ((T - 2) * L) // (T - 1) + 1

    def arrive(d):
        j = lax.rem(me - 1 - d + L, L)
        pl.when(d < L - 1)(lambda: g_copy(j, j).wait_recv())
        block = gg[j]
        own[d] = dot(rows_basis_t[...], block).astype(BF16)
        pl.when(d <= half)(lambda: end_send(d))
        wide = block.astype(F32)
        gacc[...] += jnp.sum(wide * wide, axis=0, keepdims=True)
        for h in range(1, T - 1):
            pl.when(d == (h * L) // (T - 1))(lambda h=h: c_hop(h))
        pl.when(d >= early)(lambda: forward(d - early + 1))

    loop(0, L, arrive)
    c_hop(T - 1)

    def mid_step(j):
        mid[...] += dot(gg[j], call[pl.ds(pl.multiple_of(j * W, W), W), :])

    loop(0, L, mid_step)
    core_out[...] = dot(rows_basis_t[...], mid[...].astype(BF16)).astype(BF16)

    def kp_copy(src):
        return remote(src, core_in.at[0], ks.at[0], kr.at[0], "tensor", right)

    def kq_copy(src):
        return remote(src, core_in.at[1], ks.at[1], kr.at[1], "tensor", lft)

    @pl.when(t == 0)
    def _():
        core_in[0] = jnp.zeros(core_out.shape, BF16)
        kp_copy(core_out).start()

    @pl.when(t == T - 1)
    def _():
        core_in[1] = jnp.zeros(core_out.shape, BF16)
        kq_copy(core_out).start()

    loop(half + 1, L, end_send)

    def core_step(k):
        @pl.when((k == half + t) & has_left)
        def _():
            kp_copy(core_out).wait_recv()

            @pl.when(has_right)
            def _():
                core_sum[0] = (core_in[0].astype(F32) + core_out[...].astype(F32)).astype(BF16)
                kp_copy(core_sum.at[0]).start()

        @pl.when((k == half + T - 1 - t) & has_right)
        def _():
            kq_copy(core_out).wait_recv()

            @pl.when(has_left)
            def _():
                core_sum[1] = (core_in[1].astype(F32) + core_out[...].astype(F32)).astype(BF16)
                kq_copy(core_sum.at[1]).start()

    def make_left():
        core = core_in[0].astype(F32) + core_in[1].astype(F32) + core_out[...].astype(F32)
        core = (core * dr[:, :1]).astype(BF16)
        mixed = base[0:1, 0:1] * mid[...] + dot(rows_basis[...], core)
        left[...] = (mixed * dc[0:1, :]).astype(BF16)

    def o_copy(slot, dst):
        return remote(raw_out.at[dst], out.at[slot], os_.at[dst], or_.at[slot], "layer", dst)

    def own_copy():
        return pltpu.make_async_copy(raw_out.at[me], out.at[me], os_.at[me])

    def emit(d):
        j = lax.rem(me - 1 - d + L, L)
        total = own[d].astype(F32) + pin[d].astype(F32) + qin[d].astype(F32)
        scaled = (total * dr[:, :1]).astype(BF16)
        raw = base[2:3, 0:1] * gg[j].astype(F32)
        raw = raw + base[1:2, 0:1] * dot(rows_basis[...], scaled)
        raw = raw + lax.dot_general(
            left[...], call[pl.ds(pl.multiple_of(j * W, W), W), :],
            (((1,), (1,)), ((), ())), preferred_element_type=F32)
        raw_out[j] = raw.astype(BF16)
        pl.when(d == L - 1)(lambda: own_copy().start())
        pl.when(d < L - 1)(lambda: o_copy(me, j).start())
        uacc[...] += jnp.sum(raw * raw, axis=0, keepdims=True)

    first = half + T - 1

    def upto(k):
        paced = jnp.minimum(k - T + 2, 3 + 2 * (k - first))
        return jnp.where(has_left & has_right, paced, k - T + 2)

    def tail_step(k):
        core_step(k)
        forward(k)
        pl.when(k == first)(make_left)
        pl.when(k == first)(lambda: loop(0, upto(k), emit))
        pl.when(k > first)(lambda: loop(upto(k - 1), upto(k), emit))

    loop(L - early + 1, L + T - 1, tail_step)

    nsend[0:8, :] = jnp.broadcast_to(jnp.sum(gacc[...]), (8, 128))
    nsend[8:16, :] = jnp.broadcast_to(jnp.sum(uacc[...]), (8, 128))

    def n_copy(slot, dst):
        return remote(nsend, nrecv.at[slot], ns.at[dst], nr.at[slot], "tensor", dst)

    loop(1, T, lambda d: n_copy(t, lax.rem(t + d, T)).start())
    nrecv[t] = nsend[...]
    for d in range(1, T):
        s = lax.rem(t + d, T)
        n_copy(s, s).wait_recv()
    sq = nrecv[0]
    for s in range(1, T):
        sq = sq + nrecv[s]
    fsend[...] = jnp.sqrt((sq[0:8] + 1.0) / (sq[8:16] + 1.0))

    def f_copy(slot, dst):
        return remote(fsend, frecv.at[slot], fs.at[dst], fr.at[slot], "layer", dst)

    loop(1, L, lambda d: f_copy(me, lax.rem(me + d, L)).start())
    frecv[me] = fsend[...]
    own_copy().wait()

    def finish(d):
        j = lax.rem(me + d, L)
        o_copy(j, j).wait_recv()
        f_copy(j, j).wait_recv()

    loop(1, L, finish)
    factor[...] = frecv[...]

    def drain_layer(d):
        j = lax.rem(me + d, L)
        g_copy(me, j).wait_send()
        o_copy(me, j).wait_send()
        f_copy(me, j).wait_send()

    loop(1, L, drain_layer)
    pl.when(has_right)(lambda: kp_copy(core_out).wait_send())
    pl.when(has_left)(lambda: kq_copy(core_out).wait_send())

    def drain_tensor(d):
        s = lax.rem(t + d, T)
        n_copy(t, s).wait_send()

    loop(1, T, drain_tensor)

    def drain_line(d):
        pl.when(has_right)(lambda: p_copy(own.at[d], d).wait_send())
        pl.when(has_left)(lambda: q_copy(own.at[d], d).wait_send())

    loop(0, L, drain_line)
    for h in range(T - 1):
        pl.when((t - h >= 0) & has_right)(lambda h=h: c_copy(cols, t, h, 0).wait_send())
        pl.when((t + h < T) & has_left)(lambda h=h: c_copy(cols, t, h, 1).wait_send())


def solution(mesh):
    L, T = mesh.shape["layer"], mesh.shape["tensor"]

    def body(gradient, row_basis, column_basis, row_eigen, column_eigen, row_escape, column_escape):
        row_base = row_escape ** (-0.25)
        column_base = column_escape ** (-0.25)
        row_coef = (row_eigen + row_escape[:, None]) ** (-0.25) - row_base[:, None]
        column_coef = (column_eigen + column_escape[:, None]) ** (-0.25) - column_base[:, None]
        _, r, W = gradient.shape
        _, Cr, K = column_basis.shape
        dr = jnp.broadcast_to(row_coef[0][:, None], (K, 128))
        dc = jnp.broadcast_to(column_coef, (8, K))
        base = jnp.broadcast_to(
            jnp.concatenate([row_base, column_base, row_base * column_base] + [row_base] * 5)[:, None], (8, 128))
        vmem = pl.BlockSpec(memory_space=pltpu.VMEM)
        chunk = pltpu.VMEM((L, K, W), BF16)
        block = pltpu.VMEM((L, r, W), BF16)
        sem = pltpu.SemaphoreType.DMA
        raw, factor = pl.pallas_call(
            functools.partial(kernel, L, T),
            out_shape=(jax.ShapeDtypeStruct((L, r, W), BF16), jax.ShapeDtypeStruct((L, 8, 128), F32)),
            in_specs=[vmem] * 7,
            out_specs=(pl.BlockSpec(memory_space=pl.ANY), vmem),
            scratch_shapes=[
                block, chunk, chunk, chunk, chunk, chunk,
                pltpu.VMEM((T * Cr, K), BF16),
                pltpu.VMEM((r, K), F32),
                pltpu.VMEM((r, K), BF16),
                pltpu.VMEM((K, K), BF16),
                pltpu.VMEM((2, K, K), BF16),
                pltpu.VMEM((2, K, K), BF16),
                block,
                pltpu.VMEM((1, W), F32),
                pltpu.VMEM((1, W), F32),
                pltpu.VMEM((16, 128), F32),
                pltpu.VMEM((T, 16, 128), F32),
                pltpu.VMEM((8, 128), F32),
                pltpu.VMEM((L, 8, 128), F32),
                sem((L,)), sem((L,)),
                sem((2, T)), sem((T,)),
                sem((L,)), sem((L,)),
                sem((L,)), sem((L,)),
                sem((2,)), sem((2,)),
                sem((L,)), sem((L,)),
                sem((T,)), sem((T,)),
                sem((L,)), sem((L,)),
            ],
            compiler_params=pltpu.CompilerParams(
                collective_id=0, has_side_effects=True, vmem_limit_bytes=62 * 1024 * 1024),
        )(gradient, row_basis[0], row_basis[0].T, column_basis[0], dr, dc, base)
        return (raw.astype(F32) * factor[:, :1, :1]).astype(BF16)

    in_specs = (
        P(None, "tensor", "layer"),
        P("layer", "tensor", None),
        P("layer", "tensor", None),
        P("layer", None),
        P("layer", None),
        P("layer"),
        P("layer"),
    )
    out_specs = P(None, "tensor", "layer")
    return jax.shard_map(body, mesh=mesh, in_specs=in_specs, out_specs=out_specs, check_vma=False)
```
